512 devices in a mesh: row: 64 (over y, z), col: 8 (over x, core).
Axes of the slice: x: 4, y: 4, z: 16, core: 2. Of those that a mesh axis runs over, the one named last changes fastest.
Arguments:
- sources: bfloat16 [524288, 640], P(('row', 'col')), may hold values from -6 to 6
- tree_perm: int32 [524288], P(('row', 'col')), may hold values from 0 to 524287, as said below
- leaf_blocks: bfloat16 [524288, 512], P(('row', 'col')), may hold values from -0.25 to 0.25
- u_factors: bfloat16 [10, 32, 524288], P(None, None, ('row', 'col')), may hold values from -0.3125 to 0.3125
- v_factors: bfloat16 [10, 32, 524288], P(None, None, ('row', 'col')), as said below
- level_ranks: int32 [10], replicated, may hold values from 16 to 32
Outputs:
- products: bfloat16 [524288, 640], P(('row', 'col'))
The draws below stay inside these ranges and needn't reach their ends.
Inputs may be any that keep to these rules, and one draw needn't show every extreme that they name: tree_perm is a permutation that maps each aligned block of 1024 positions onto the same block of initial indices. `v_factors`: entries of level l are of the order of the inverse square root of 524288 / 2^l.
All inputs are finite; a program needn't handle non-finite values.
Results may differ from the reference program's by a relative error of at most 0.0037.
Values sent between devices are 32-bit elements; how exact they have to be, the bound alone decides.
A program may use at most 64 MiB of HBM per device.

```python
import jax
import jax.numpy as jnp
from jax import lax

LEAF = 512
K = 32
RHS = 640
ROWS_DEV = 1024
N = 524288
LEVELS = 10


def draw_tree_perm(key, part):
    blocks = N // ROWS_DEV
    keys = jax.random.split(key, blocks)
    perms = jax.vmap(lambda one_key: jax.random.permutation(one_key, ROWS_DEV))(keys).astype(jnp.int32)
    offsets = jnp.arange(blocks, dtype=jnp.int32)[:, None] * ROWS_DEV
    return (perms + offsets).reshape(N).astype(jnp.int32)


def draw_v_factors(key, part):
    level_scale = jnp.sqrt(2.0 ** (jnp.arange(LEVELS, dtype=jnp.float32) + 1.0) / N)
    base = jax.random.normal(key, (LEVELS, K, N), jnp.float32)
    return (base * level_scale[:, None, None]).astype(jnp.bfloat16)


def set_ends(array, stream_key, low, top_value):
    shape = array.shape
    place = [jax.random.randint(jax.random.fold_in(stream_key, axis), (), 0, shape[axis]) for axis in range(len(shape))]
    array = array.at[tuple(place)].set(low)
    longest = shape.index(max(shape))
    place[longest] = (place[longest] + 1) % shape[longest]
    return array.at[tuple(place)].set(top_value)


def levels(rng, extent, cuts, smallest, largest):
    level = 1.0
    for dim, blocks in cuts:
        steps = jax.random.uniform(jax.random.fold_in(jax.random.fold_in(rng, 6), dim), (blocks,), jnp.float32, smallest / len(cuts), largest / len(cuts))
        level = level * jnp.repeat(jnp.exp(steps), extent[dim] // blocks).reshape((-1,) + (1,) * (len(extent) - 1 - dim))
    return level


def bell_draw(stream_key, shape, width, most, cuts=(), held_as=jnp.bfloat16):
    array = width * jax.random.normal(stream_key, shape, jnp.float32)
    if cuts:
        array = array * levels(stream_key, shape, cuts, -0.22, 0.18)
    return jnp.clip(array, -most, most).astype(held_as)


def setup_inputs(seed: int = 0) -> dict:
    arg_keys = jax.random.split(jax.random.key(seed), 7)
    return {
        "sources": bell_draw(arg_keys[0], (N, RHS), 1.0, 6.0, ((0, 512),)),
        "tree_perm": draw_tree_perm(jax.random.fold_in(arg_keys[6], 71), 0),
        "leaf_blocks": bell_draw(arg_keys[2], (N, LEAF), LEAF ** -0.5, 0.25, ((0, 512),)),
        "u_factors": bell_draw(arg_keys[3], (LEVELS, K, N), (K * LEVELS) ** -0.5, 0.3125, ((2, 512),)),
        "v_factors": draw_v_factors(jax.random.fold_in(arg_keys[6], 71), 0),
        "level_ranks": set_ends(jax.random.randint(arg_keys[5], (LEVELS,), K // 2, K + 1), jax.random.fold_in(arg_keys[5], 1), K // 2, K).astype(jnp.int32),
    }


def reference(sources, tree_perm, leaf_blocks, u_factors, v_factors, level_ranks):
    ordered = sources[tree_perm].astype(jnp.float32)
    leaf_count = N // LEAF
    result = jnp.einsum("gij,gjr->gir", leaf_blocks.reshape(leaf_count, LEAF, LEAF).astype(jnp.float32), ordered.reshape(leaf_count, LEAF, RHS)).reshape(N, RHS)
    rank_index = lax.iota(jnp.int32, K)
    for level in range(LEVELS):
        groups = 2 ** (level + 1)
        cluster_rows = N // groups
        v_level = v_factors[level].astype(jnp.float32).reshape(K, groups, cluster_rows)
        coef = jnp.einsum("kgs,gsr->gkr", v_level, ordered.reshape(groups, cluster_rows, RHS))
        far_coef = coef.reshape(groups // 2, 2, K, RHS)[:, ::-1].reshape(groups, K, RHS)
        rank_mask = (rank_index < level_ranks[level]).astype(jnp.float32)
        far_coef = (far_coef * rank_mask[None, :, None]).astype(jnp.bfloat16).astype(jnp.float32)
        u_level = u_factors[level].astype(jnp.float32).reshape(K, groups, cluster_rows)
        result = result + jnp.einsum("kgs,gkr->gsr", u_level, far_coef).reshape(N, RHS)
    tree_out = result.astype(jnp.bfloat16)
    return jnp.zeros((N, RHS), jnp.bfloat16).at[tree_perm].set(tree_out)
```

```python
import functools

import jax
import jax.numpy as jnp
from jax import lax
from jax.experimental import pallas as pl
from jax.experimental.pallas import tpu as pltpu
from jax.sharding import Mesh
from jax.sharding import PartitionSpec as P

AXES = ("y", "z", "x", "c")
MESH_ID = pl.DeviceIdType.MESH
NT = (((1,), (1,)), ((), ()))
TN = (((0,), (0,)), ((), ()))
NN = (((1,), (0,)), ((), ()))
F32 = jnp.float32
BF16 = jnp.bfloat16
RANK = 32
RHS = 640
ROWS = 1024
LEAF = 512
STEP = 128


def dot(a, b, dims=NN):
    return lax.dot_general(a, b, dims, preferred_element_type=F32)


def flip(v, mask):
    out, bit = v, 1
    while bit <= mask:
        if mask & bit:
            out = out + bit - 2 * bit * ((v // bit) % 2)
        bit *= 2
    return out


def kernel(
    perm_ref, ranks_ref, src_hbm, leaf_hbm, u_hbm, v_hbm, out_hbm,
    src, leaf, u, v, pt, vp, uperm, up_far, up_near, ordered, leaf_rows, near_far, acc, out,
    coef, core_in, twin_in, xs, xin, six, seven, pair_out, pair_in,
    n0, n1, n23, in0, in1, in23, four_in, five_in, fs, far_in, quad, quad_in, e0, e0_in, e1, e1_in,
    load_sem, out_sem, send_sem, recv_sem,
):
    y, z, x, c = (lax.axis_index(name) for name in AXES)
    zq = z % 4

    count = [0]
    started = []

    def target(dy=0, dz=0, dx=0, dc=0):
        return (flip(y, dy), flip(z, dz), flip(x, dx), flip(c, dc))

    def send(source, dest, **by):
        k = count[0]
        count[0] += 1
        copy = pltpu.make_async_remote_copy(
            src_ref=source, dst_ref=dest, send_sem=send_sem.at[k], recv_sem=recv_sem.at[k],
            device_id=target(**by), device_id_type=MESH_ID,
        )
        copy.start()
        started.append(copy)
        return copy

    loads = []
    for k, (a, b) in enumerate(((v_hbm, v), (src_hbm, src), (leaf_hbm, leaf), (u_hbm, u))):
        copy = pltpu.make_async_copy(a, b, load_sem.at[k])
        copy.start()
        loads.append(copy)

    partners = [dict(dc=1)]
    partners += [dict(dx=d, dc=e) for d in (1, 2, 3) for e in (0, 1)]
    partners += [dict(dy=a, dz=b) for a in range(4) for b in range(4) if a or b]
    partners += [dict(dz=d) for d in (4, 8, 12)]
    barrier = pltpu.get_barrier_semaphore()
    for by in partners:
        pl.semaphore_signal(barrier, inc=1, device_id=target(**by), device_id_type=MESH_ID)

    first_row = (((y * 16 + z) * 4 + x) * 2 + c) * ROWS
    local = perm_ref[...] - first_row

    def one_hot(k, _):
        rows = lax.broadcasted_iota(jnp.int32, (STEP, ROWS), 0) + k * STEP
        at = pl.ds(pl.multiple_of(k * STEP, STEP), STEP)
        pt[at, :] = jnp.where(rows == local, 1.0, 0.0).astype(BF16)
        return 0

    lax.fori_loop(0, ROWS // STEP, one_hot, 0)
    loads[0].wait()
    for k in range(4):
        at = slice(k * 256, k * 256 + 256)
        vp[:, at] = dot(v[0:288, :], pt[at, :], NT).astype(BF16)
    loads[1].wait()
    for n in range(5):
        cols = slice(n * 128, n * 128 + 128)
        coef[:, :, :, cols] = dot(vp[...], src[:, cols]).reshape(9, 2, 16, 128)

    pl.semaphore_wait(barrier, len(partners))

    core_a = send(coef.at[0:2, 1 - c], core_in.at[0:2], dc=1)
    core_b = send(coef.at[2:8, 1 - c], core_in.at[2:8], dc=1)
    twin = send(coef.at[8], twin_in, dc=1)

    def chip_sum(level):
        total = coef[level, c] + core_in[level]
        for q in range(4):
            xs[q, level] = total[4 * q : 4 * q + 4]

    core_a.wait_recv()
    for level in (0, 1):
        chip_sum(level)
    x_a = [send(xs.at[flip(x, d), 0:2], xin.at[d - 1, 0:2], dx=d) for d in (1, 2, 3)]
    core_b.wait_recv()
    for level in (2, 3, 4, 5):
        chip_sum(level)
    x_b = [send(xs.at[flip(x, d), 2:6], xin.at[d - 1, 2:6], dx=d) for d in (1, 2, 3)]
    for k in (0, 1):
        pair_out[k] = coef[6 + k, c] + core_in[6 + k]
    six_in = [send(pair_out.at[0], six.at[d - 2], dx=d) for d in (2, 3)]
    seven_in = send(pair_out.at[1], seven, dx=1)

    def row_sum(level):
        return ((xs[x, level] + xin[0, level]) + xin[1, level]) + xin[2, level]

    for copy in x_a:
        copy.wait_recv()
    for level, held in ((0, n0), (1, n1)):
        total = row_sum(level)
        for q in range(4):
            held[q] = total[q : q + 1]
    near = [send(n0.at[flip(zq, b)], in0.at[(a - 2) * 4 + b], dy=a, dz=b) for a in (2, 3) for b in range(4)]
    near += [send(n1.at[flip(zq, b)], in1.at[b], dy=1, dz=b) for b in range(4)]
    for copy in x_b:
        copy.wait_recv()
    for k, level in ((0, 2), (1, 3)):
        total = row_sum(level)
        for q in range(4):
            n23[q, k] = total[q : q + 1]
    near += [send(n23.at[flip(zq, b)], in23.at[b - 1], dz=b) for b in (1, 2, 3)]
    e1[0:4] = row_sum(4)
    e1[4:8] = row_sum(5)
    fours = [send(e1.at[0:4], four_in.at[d - 2], dz=d) for d in (2, 3)]
    fives = send(e1.at[4:8], five_in, dz=1)

    for copy in near:
        copy.wait_recv()
    total = in0[0]
    for k in range(1, 8):
        total = total + in0[k]
    fs[1] = total
    fs[2] = ((in1[0] + in1[1]) + in1[2]) + in1[3]
    for k, slot in ((0, 3), (1, 0)):
        fs[slot] = ((n23[zq, k] + in23[0, k]) + in23[1, k]) + in23[2, k]
    far = [send(fs.at[0:3], far_in.at[0], dz=4)]
    far += [send(fs.at[1:4], far_in.at[d], dz=4 + 4 * d) for d in (1, 2)]

    for copy in six_in:
        copy.wait_recv()
    seven_in.wait_recv()
    pair_in[0, 0] = six[0] + six[1]
    pair_in[0, 1] = seven[...]
    pair_copy = send(pair_in.at[0], pair_in.at[1], dc=1)
    for copy in fours:
        copy.wait_recv()
    fives.wait_recv()
    e1_in[0, 0:4] = four_in[0] + four_in[1]
    e1_in[0, 4:8] = five_in[...]
    shares = [(d, e) for d in range(4) for e in range(2) if d or e]
    e1_copies = [send(e1_in.at[0], e1_in.at[d * 2 + e], dx=d, dc=e) for d, e in shares]

    loads[2].wait()
    loads[3].wait()

    def ordered_step(k, _):
        at = pl.ds(pl.multiple_of(k * STEP, STEP), STEP)
        ordered[at, :] = dot(pt[:, at], src[...], TN).astype(BF16)
        return 0

    lax.fori_loop(0, ROWS // STEP, ordered_step, 0)

    def rank_rows(level, limit_shape):
        out_rank = jnp.zeros(limit_shape, jnp.int32)
        for k in range(10):
            out_rank = jnp.where(level == k, ranks_ref[k], out_rank)
        return out_rank

    shape = (288, 288)
    row = lax.broadcasted_iota(jnp.int32, shape, 0)
    col = lax.broadcasted_iota(jnp.int32, shape, 1)
    slot_a, inner_a = row >> 4, row & 15
    level_a = inner_a & 3
    k_a = 16 * (c ^ (slot_a & 1)) + 4 * (x ^ (slot_a >> 1)) + (zq ^ (inner_a >> 2))
    row_b = row - 128
    slot_b, inner_b = row_b >> 3, row_b & 7
    level_b = 4 + (inner_b >> 2)
    k_b = 16 * (c ^ (slot_b & 1)) + 4 * (x ^ (slot_b >> 1)) + (inner_b & 3)
    row_c = row - 192
    level_c = 6 + ((row_c >> 4) & 1)
    k_c = 16 * (c ^ (row_c >> 5)) + (row_c & 15)
    row_d = row - 256
    level = jnp.where(row < 128, level_a, jnp.where(row < 192, level_b, jnp.where(row < 256, level_c, 8)))
    k_of = jnp.where(row < 128, k_a, jnp.where(row < 192, k_b, jnp.where(row < 256, k_c, row_d)))
    keep = (col == level * RANK + k_of) & (k_of < rank_rows(level, shape))
    pick = jnp.where(keep, 1.0, 0.0).astype(BF16)
    for n in range(4):
        at = slice(n * 256, n * 256 + 256)
        uperm[0:288, at] = dot(pick, u[0:288, at]).astype(BF16)
    shape = (RANK, LEAF)
    live = lax.broadcasted_iota(jnp.int32, shape, 0) < ranks_ref[9]
    zeros = jnp.zeros(shape, BF16)
    uperm[288:320, 0:LEAF] = jnp.where(live, u[288:320, 0:LEAF], zeros)
    uperm[288:320, LEAF:] = zeros
    uperm[320:352, 0:LEAF] = zeros
    uperm[320:352, LEAF:] = jnp.where(live, u[288:320, LEAF:], zeros)

    def up_step(k, _):
        at = pl.ds(pl.multiple_of(k * STEP, STEP), STEP)
        up_far[at, :] = dot(pt[at, :], uperm[0:128, :], NT).astype(BF16)
        up_near[at, :] = dot(pt[at, :], uperm[128:352, :], NT).astype(BF16)
        for g in range(2):
            cols = slice(g * LEAF, g * LEAF + LEAF)
            leaf_rows[at, cols] = dot(pt[at, cols], leaf[cols, :]).astype(BF16)
        return 0

    lax.fori_loop(0, ROWS // STEP, up_step, 0)

    for g in range(2):
        other = slice((1 - g) * LEAF, (1 - g) * LEAF + LEAF)
        got = dot(v[288:320, other], ordered[other, :])
        near_far[160 + 32 * g : 192 + 32 * g, :] = got.astype(BF16)
    twin.wait_recv()
    near_far[128:160, :] = twin_in[...].reshape(32, RHS).astype(BF16)
    pair_copy.wait_recv()
    near_far[64:128, :] = pair_in[...].reshape(64, RHS).astype(BF16)
    for copy in e1_copies:
        copy.wait_recv()
    near_far[0:64, :] = e1_in[...].reshape(64, RHS).astype(BF16)

    def acc_step(k, _):
        at = pl.ds(pl.multiple_of(k * STEP, STEP), STEP)
        acc[at, :] = dot(leaf_rows[at, :], ordered[...]) + dot(up_near[at, :], near_far[...])
        return 0

    lax.fori_loop(0, ROWS // STEP, acc_step, 0)

    for copy in far:
        copy.wait_recv()
    quad[0] = ((fs[1] + far_in[0, 1]) + far_in[1, 0]) + far_in[2, 0]
    quad[1] = ((fs[2] + far_in[0, 2]) + far_in[1, 1]) + far_in[2, 1]
    quad[2] = far_in[1, 2] + far_in[2, 2]
    quad[3] = far_in[0, 0]
    quads = [send(quad, quad_in.at[b - 1], dz=b) for b in (1, 2, 3)]
    for k in range(4):
        e0[k : k + 1] = quad[k]
    for copy in quads:
        copy.wait_recv()
    for b in (1, 2, 3):
        for k in range(4):
            e0[4 * b + k : 4 * b + k + 1] = quad_in[b - 1, k]
    e0_copies = [send(e0, e0_in.at[d * 2 + e], dx=d, dc=e) for d, e in shares]
    e0_in[0] = e0[...]
    for copy in e0_copies:
        copy.wait_recv()
    far_rows = e0_in[...].reshape(128, RHS).astype(BF16)

    for k in range(ROWS // STEP):
        at = slice(k * STEP, k * STEP + STEP)
        out[at, :] = (acc[at, :] + dot(up_far[at, :], far_rows)).astype(BF16)
        pltpu.make_async_copy(out.at[at], out_hbm.at[at], out_sem.at[k]).start()
    for copy in started:
        copy.wait_send()
    for k in range(ROWS // STEP):
        at = slice(k * STEP, k * STEP + STEP)
        pltpu.make_async_copy(out.at[at], out_hbm.at[at], out_sem.at[k]).wait()


def per_device(sources, tree_perm, leaf_blocks, u_factors, v_factors, level_ranks):
    vmem = pltpu.VMEM
    copies = 80
    scratch = [
        vmem((ROWS, RHS), BF16), vmem((ROWS, LEAF), BF16), vmem((320, ROWS), BF16), vmem((320, ROWS), BF16),
        vmem((ROWS, ROWS), BF16), vmem((288, ROWS), BF16), vmem((352, ROWS), BF16),
        vmem((ROWS, 128), BF16), vmem((ROWS, 224), BF16), vmem((ROWS, RHS), BF16), vmem((ROWS, ROWS), BF16),
        vmem((224, RHS), BF16), vmem((ROWS, RHS), F32), vmem((ROWS, RHS), BF16),
        vmem((9, 2, 16, RHS), F32), vmem((8, 16, RHS), F32), vmem((2, 16, RHS), F32),
        vmem((4, 6, 4, RHS), F32), vmem((3, 6, 4, RHS), F32), vmem((2, 16, RHS), F32), vmem((16, RHS), F32),
        vmem((2, 16, RHS), F32), vmem((2, 2, 16, RHS), F32),
        vmem((4, 1, RHS), F32), vmem((4, 1, RHS), F32), vmem((4, 2, 1, RHS), F32),
        vmem((8, 1, RHS), F32), vmem((4, 1, RHS), F32), vmem((3, 2, 1, RHS), F32),
        vmem((2, 4, RHS), F32), vmem((4, RHS), F32), vmem((4, 1, RHS), F32), vmem((3, 3, 1, RHS), F32),
        vmem((4, 1, RHS), F32), vmem((3, 4, 1, RHS), F32), vmem((16, RHS), F32), vmem((8, 16, RHS), F32),
        vmem((8, RHS), F32), vmem((8, 8, RHS), F32),
        pltpu.SemaphoreType.DMA((4,)), pltpu.SemaphoreType.DMA((8,)),
        pltpu.SemaphoreType.DMA((copies,)), pltpu.SemaphoreType.DMA((copies,)),
    ]
    anywhere = pl.BlockSpec(memory_space=pl.ANY)
    return pl.pallas_call(
        kernel,
        out_shape=jax.ShapeDtypeStruct((ROWS, RHS), BF16),
        in_specs=[
            pl.BlockSpec(memory_space=pltpu.VMEM), pl.BlockSpec(memory_space=pltpu.SMEM),
            anywhere, anywhere, anywhere, anywhere,
        ],
        out_specs=anywhere,
        scratch_shapes=scratch,
        compiler_params=pltpu.CompilerParams(
            collective_id=0, has_side_effects=True, vmem_limit_bytes=60 * 1024 * 1024
        ),
    )(
        tree_perm.reshape(1, ROWS), level_ranks, sources, leaf_blocks,
        u_factors.reshape(320, ROWS), v_factors.reshape(320, ROWS),
    )


def solution(mesh):
    torus = Mesh(mesh.devices.reshape(4, 16, 4, 2), AXES)
    placed = (P(AXES, None), P(AXES), P(AXES, None), P(None, None, AXES), P(None, None, AXES), P())
    return jax.shard_map(per_device, mesh=torus, in_specs=placed, out_specs=P(AXES, None), check_vma=False)
```

```python
import functools

import jax
import jax.numpy as jnp
from jax import lax
from jax.experimental import pallas as pl
from jax.experimental.pallas import tpu as pltpu
from jax.sharding import Mesh
from jax.sharding import PartitionSpec as P

AXES = ("y", "z", "x", "c")
MESH_ID = pl.DeviceIdType.MESH
NT = (((1,), (1,)), ((), ()))
TN = (((0,), (0,)), ((), ()))
NN = (((1,), (0,)), ((), ()))
F32 = jnp.float32
BF16 = jnp.bfloat16
RANK = 32
RHS = 640
ROWS = 1024
LEAF = 512
STEP = 128
BLOCK = 256


def dot(a, b, dims=NN):
    return lax.dot_general(a, b, dims, preferred_element_type=F32)


def flip(v, mask):
    out, bit = v, 1
    while bit <= mask:
        if mask & bit:
            out = out + bit - 2 * bit * ((v // bit) % 2)
        bit *= 2
    return out


def kernel(
    perm_hbm, ranks_ref, src_hbm, leaf_hbm, u_hbm, v_hbm, acc, up_far, far_rows,
    perm, src, leaf, u, v, pt, vp, uperm, up_near, ordered, leaf_rows, near_far,
    coef, core_in, twin_in, xs, xin, six, seven, pair_out, pair_in,
    n0, n1, n23, in0, in1, in23, four_in, five_in, fs, far_in, quad, quad_in, e0_in, e1, e1_in,
    load_sem, send_sem, recv_sem,
):
    y, z, x, c = (lax.axis_index(name) for name in AXES)
    zq = z % 4

    count = [0]
    started = []

    def target(dy=0, dz=0, dx=0, dc=0):
        return (flip(y, dy), flip(z, dz), flip(x, dx), flip(c, dc))

    def send(source, dest, **by):
        k = count[0]
        count[0] += 1
        copy = pltpu.make_async_remote_copy(
            src_ref=source, dst_ref=dest, send_sem=send_sem.at[k], recv_sem=recv_sem.at[k],
            device_id=target(**by), device_id_type=MESH_ID,
        )
        copy.start()
        started.append(copy)
        return copy

    partners = [dict(dc=1)]
    partners += [dict(dx=d) for d in (1, 2, 3)]
    partners += [dict(dy=a, dz=b) for a in range(4) for b in range(4) if a or b]
    partners += [dict(dz=d) for d in (4, 8, 12)]
    barrier = pltpu.get_barrier_semaphore()
    for by in partners:
        pl.semaphore_signal(barrier, inc=1, device_id=target(**by), device_id_type=MESH_ID)

    loads = []

    def load(a, b):
        copy = pltpu.make_async_copy(a, b, load_sem.at[len(loads)])
        copy.start()
        loads.append(copy)
        return copy

    perm_load = load(perm_hbm, perm)
    v_first = load(v_hbm.at[0:128], v.at[0:128])
    src_loads = [load(src_hbm.at[k : k + 256], src.at[k : k + 256]) for k in range(0, ROWS, 256)]
    v_rest = load(v_hbm.at[128:320], v.at[128:320])

    first_row = (((y * 16 + z) * 4 + x) * 2 + c) * ROWS
    perm_load.wait()
    local = perm[...] - first_row

    def one_hot(k, _):
        rows = lax.broadcasted_iota(jnp.int32, (STEP, ROWS), 0) + k * STEP
        at = pl.ds(pl.multiple_of(k * STEP, STEP), STEP)
        pt[at, :] = jnp.where(rows == local, 1.0, 0.0).astype(BF16)
        return 0

    lax.fori_loop(0, ROWS // STEP, one_hot, 0)
    v_first.wait()
    for k in range(4):
        at = slice(k * 256, k * 256 + 256)
        vp[0:128, at] = dot(v[0:128, :], pt[at, :], NT).astype(BF16)
    for copy in src_loads:
        copy.wait()
    for n in range(0, RHS, 128):
        cols = slice(n, n + 128)
        coef[0:4, :, :, cols] = dot(vp[0:128, :], src[:, cols]).reshape(4, 2, 16, 128)
    leaf_load = load(leaf_hbm, leaf)
    u_load = load(u_hbm, u)

    def order_rows():
        u_load.wait()

        def ordered_step(k, _):
            at = pl.ds(pl.multiple_of(k * BLOCK, BLOCK), BLOCK)
            ordered[at, :] = dot(pt[:, at], src[...], TN).astype(BF16)
            return 0

        lax.fori_loop(0, ROWS // BLOCK, ordered_step, 0)

        shape = (288, 288)
        row = lax.broadcasted_iota(jnp.int32, shape, 0)
        col = lax.broadcasted_iota(jnp.int32, shape, 1)
        slot_a, inner_a = row >> 4, row & 15
        level_a = inner_a & 3
        k_a = 16 * (c ^ (slot_a & 1)) + 4 * (x ^ (slot_a >> 1)) + (zq ^ (inner_a >> 2))
        row_b = row - 128
        slot_b, inner_b = row_b >> 3, row_b & 7
        level_b = 4 + (inner_b >> 2)
        k_b = 16 * (c ^ (slot_b & 1)) + 4 * (x ^ (slot_b >> 1)) + (inner_b & 3)
        row_c = row - 192
        level_c = 6 + ((row_c >> 4) & 1)
        k_c = 16 * (c ^ (row_c >> 5)) + (row_c & 15)
        row_d = row - 256

        def by_part(parts):
            return jnp.where(row < 128, parts[0], jnp.where(row < 192, parts[1], jnp.where(row < 256, parts[2], parts[3])))

        level = by_part((level_a, level_b, level_c, 8))
        k_of = by_part((k_a, k_b, k_c, row_d))
        limit = jnp.zeros(shape, jnp.int32)
        for k in range(9):
            limit = jnp.where(level == k, ranks_ref[k], limit)
        keep = (col == level * RANK + k_of) & (k_of < limit)
        pick = jnp.where(keep, 1.0, 0.0).astype(BF16)
        for n in range(4):
            at = slice(n * 256, n * 256 + 256)
            uperm[0:288, at] = dot(pick, u[0:288, at]).astype(BF16)
        shape = (RANK, LEAF)
        live = lax.broadcasted_iota(jnp.int32, shape, 0) < ranks_ref[9]
        zeros = jnp.zeros(shape, BF16)
        uperm[288:320, 0:LEAF] = jnp.where(live, u[288:320, 0:LEAF], zeros)
        uperm[288:320, LEAF:] = zeros
        uperm[320:352, 0:LEAF] = zeros
        uperm[320:352, LEAF:] = jnp.where(live, u[288:320, LEAF:], zeros)

    def local_dots():
        leaf_load.wait()

        def up_step(k, _):
            at = pl.ds(pl.multiple_of(k * BLOCK, BLOCK), BLOCK)
            up_far[at, :] = dot(pt[at, :], uperm[0:128, :], NT).astype(BF16)
            up_near[at, :] = dot(pt[at, :], uperm[128:352, :], NT).astype(BF16)
            for g in range(2):
                cols = slice(g * LEAF, g * LEAF + LEAF)
                leaf_rows[at, cols] = dot(pt[at, cols], leaf[cols, :]).astype(BF16)
            return 0

        lax.fori_loop(0, ROWS // BLOCK, up_step, 0)

        def leaf_step(k, _):
            at = pl.ds(pl.multiple_of(k * BLOCK, BLOCK), BLOCK)
            acc[at, :] = dot(leaf_rows[at, :], ordered[...])
            return 0

        lax.fori_loop(0, ROWS // BLOCK, leaf_step, 0)

    pl.when(z < 8)(order_rows)
    pl.when(z < 4)(local_dots)

    pl.semaphore_wait(barrier, len(partners))

    core_a = [send(coef.at[k : k + 2, 1 - c], core_in.at[k : k + 2], dc=1) for k in (0, 2)]
    v_rest.wait()
    for k in range(4):
        at = slice(k * 256, k * 256 + 256)
        vp[128:288, at] = dot(v[128:288, :], pt[at, :], NT).astype(BF16)
    for n in range(0, RHS, 128):
        cols = slice(n, n + 128)
        coef[4:9, :, :, cols] = dot(vp[128:288, :], src[:, cols]).reshape(5, 2, 16, 128)

    def chip_sum(level):
        total = coef[level, c] + core_in[level]
        for q in range(4):
            xs[q, level] = total[4 * q : 4 * q + 4]

    def scatter_x(first):
        chip_sum(first)
        chip_sum(first + 1)
        return [send(xs.at[flip(x, d), first : first + 2], xin.at[d - 1, first : first + 2], dx=d) for d in (1, 2, 3)]

    def row_sum(level):
        return ((xs[x, level] + xin[0, level]) + xin[1, level]) + xin[2, level]

    core_a[0].wait_recv()
    x_a = scatter_x(0)
    core_a[1].wait_recv()
    x_b = scatter_x(2)
    core_b = send(coef.at[4:8, 1 - c], core_in.at[4:8], dc=1)
    twin = send(coef.at[8], twin_in, dc=1)

    for copy in x_a:
        copy.wait_recv()
    for level, held in ((0, n0), (1, n1)):
        total = row_sum(level)
        for q in range(4):
            held[q] = total[q : q + 1]
    near = [send(n0.at[flip(zq, b)], in0.at[(a - 2) * 4 + b], dy=a, dz=b) for a in (2, 3) for b in range(4)]
    near += [send(n1.at[flip(zq, b)], in1.at[b], dy=1, dz=b) for b in range(4)]
    for copy in x_b:
        copy.wait_recv()
    for k, level in ((0, 2), (1, 3)):
        total = row_sum(level)
        for q in range(4):
            n23[q, k] = total[q : q + 1]
    near += [send(n23.at[flip(zq, b)], in23.at[b - 1], dz=b) for b in (1, 2, 3)]

    core_b.wait_recv()
    x_c = scatter_x(4)
    for k in (0, 1):
        pair_out[k] = coef[6 + k, c] + core_in[6 + k]
    six_in = [send(pair_out.at[0], six.at[d - 2], dx=d) for d in (2, 3)]
    seven_in = send(pair_out.at[1], seven, dx=1)

    for copy in near:
        copy.wait_recv()
    total = in0[0]
    for k in range(1, 8):
        total = total + in0[k]
    fs[1] = total
    fs[2] = ((in1[0] + in1[1]) + in1[2]) + in1[3]
    for k, slot in ((0, 3), (1, 0)):
        fs[slot] = ((n23[zq, k] + in23[0, k]) + in23[1, k]) + in23[2, k]
    far = [send(fs.at[1:4], far_in.at[d], dz=4 + 4 * d) for d in (1, 2)]
    far += [send(fs.at[0:3], far_in.at[0], dz=4)]

    for copy in x_c:
        copy.wait_recv()
    e1[0:4] = row_sum(4)
    e1[4:8] = row_sum(5)
    fours = [send(e1.at[0:4], four_in.at[d - 2], dz=d) for d in (2, 3)]
    fives = send(e1.at[4:8], five_in, dz=1)
    for copy in six_in:
        copy.wait_recv()
    seven_in.wait_recv()
    pair_in[0, 0] = six[0] + six[1]
    pair_in[0, 1] = seven[...]
    pair_copy = send(pair_in.at[0], pair_in.at[1], dc=1)
    for copy in fours:
        copy.wait_recv()
    fives.wait_recv()
    e1_in[0, 0:4] = four_in[0] + four_in[1]
    e1_in[0, 4:8] = five_in[...]

    def share(held):
        to_twin = [send(held.at[0], held.at[1], dc=1)]
        across = [send(held.at[0], held.at[2 * d], dx=d) for d in (1, 3, 2)]
        return to_twin, across

    def relay(held, parts):
        to_twin, across = parts
        for copy, d in zip(across, (1, 3, 2)):
            copy.wait_recv()
            to_twin.append(send(held.at[2 * d], held.at[2 * d + 1], dc=1))
        for copy in to_twin:
            copy.wait_recv()

    e1_parts = share(e1_in)
    pl.when(z >= 8)(order_rows)
    pl.when(z >= 4)(local_dots)

    for copy in far:
        copy.wait_recv()
    quad[0] = ((fs[1] + far_in[0, 1]) + far_in[1, 0]) + far_in[2, 0]
    quad[1] = ((fs[2] + far_in[0, 2]) + far_in[1, 1]) + far_in[2, 1]
    quad[2] = far_in[1, 2] + far_in[2, 2]
    quad[3] = far_in[0, 0]
    quads = [send(quad, quad_in.at[b - 1], dz=b) for b in (3, 2, 1)]
    relay(e1_in, e1_parts)
    for k in range(4):
        e0_in[0, k : k + 1] = quad[k]
    for copy in quads:
        copy.wait_recv()
    for b in (1, 2, 3):
        for k in range(4):
            e0_in[0, 4 * b + k : 4 * b + k + 1] = quad_in[b - 1, k]
    e0_parts = share(e0_in)

    for g in range(2):
        other = slice((1 - g) * LEAF, (1 - g) * LEAF + LEAF)
        got = dot(v[288:320, other], ordered[other, :])
        near_far[160 + 32 * g : 192 + 32 * g, :] = got.astype(BF16)
    twin.wait_recv()
    near_far[128:160, :] = twin_in[...].reshape(32, RHS).astype(BF16)
    pair_copy.wait_recv()
    near_far[64:128, :] = pair_in[...].reshape(64, RHS).astype(BF16)
    near_far[0:64, :] = e1_in[...].reshape(64, RHS).astype(BF16)

    def acc_step(k, _):
        at = pl.ds(pl.multiple_of(k * BLOCK, BLOCK), BLOCK)
        acc[at, :] = acc[at, :] + dot(up_near[at, :], near_far[...])
        return 0

    lax.fori_loop(0, ROWS // BLOCK, acc_step, 0)

    relay(e0_in, e0_parts)
    far_rows[...] = e0_in[...].reshape(128, RHS).astype(BF16)
    for copy in started:
        copy.wait_send()


def last(acc, up_far, far_rows, out_hbm, out, out_sem):
    copies = []
    for k in range(ROWS // STEP):
        at = slice(k * STEP, k * STEP + STEP)
        out[at, :] = (acc[at, :] + dot(up_far[at, :], far_rows[...])).astype(BF16)
        copies.append(pltpu.make_async_copy(out.at[at], out_hbm.at[at], out_sem.at[k]))
        copies[-1].start()
    for copy in copies:
        copy.wait()


def per_device(sources, tree_perm, leaf_blocks, u_factors, v_factors, level_ranks):
    vmem = pltpu.VMEM
    copies = 64
    scratch = [
        vmem((1, ROWS), jnp.int32),
        vmem((ROWS, RHS), BF16), vmem((ROWS, LEAF), BF16), vmem((320, ROWS), BF16), vmem((320, ROWS), BF16),
        vmem((ROWS, ROWS), BF16), vmem((288, ROWS), BF16), vmem((352, ROWS), BF16),
        vmem((ROWS, 224), BF16), vmem((ROWS, RHS), BF16), vmem((ROWS, ROWS), BF16), vmem((224, RHS), BF16),
        vmem((9, 2, 16, RHS), F32), vmem((8, 16, RHS), F32), vmem((2, 16, RHS), F32),
        vmem((4, 6, 4, RHS), F32), vmem((3, 6, 4, RHS), F32), vmem((2, 16, RHS), F32), vmem((16, RHS), F32),
        vmem((2, 16, RHS), F32), vmem((2, 2, 16, RHS), F32),
        vmem((4, 1, RHS), F32), vmem((4, 1, RHS), F32), vmem((4, 2, 1, RHS), F32),
        vmem((8, 1, RHS), F32), vmem((4, 1, RHS), F32), vmem((3, 2, 1, RHS), F32),
        vmem((2, 4, RHS), F32), vmem((4, RHS), F32), vmem((4, 1, RHS), F32), vmem((3, 3, 1, RHS), F32),
        vmem((4, 1, RHS), F32), vmem((3, 4, 1, RHS), F32), vmem((8, 16, RHS), F32),
        vmem((8, RHS), F32), vmem((8, 8, RHS), F32),
        pltpu.SemaphoreType.DMA((9,)), pltpu.SemaphoreType.DMA((copies,)), pltpu.SemaphoreType.DMA((copies,)),
    ]
    anywhere = pl.BlockSpec(memory_space=pltpu.HBM)
    inside = pl.BlockSpec(memory_space=vmem)
    held = pl.pallas_call(
        kernel,
        out_shape=(vmem((ROWS, RHS), F32), vmem((ROWS, 128), BF16), vmem((128, RHS), BF16)),
        in_specs=[anywhere, pl.BlockSpec(memory_space=pltpu.SMEM), anywhere, anywhere, anywhere, anywhere],
        out_specs=(inside, inside, inside),
        scratch_shapes=scratch,
        compiler_params=pltpu.CompilerParams(
            collective_id=0, has_side_effects=True, vmem_limit_bytes=63_800_000
        ),
    )(
        tree_perm.reshape(1, ROWS), level_ranks, sources, leaf_blocks,
        u_factors.reshape(320, ROWS), v_factors.reshape(320, ROWS),
    )
    held = [pltpu.with_memory_space_constraint(a, vmem) for a in held]
    return pl.pallas_call(
        last,
        out_shape=jax.ShapeDtypeStruct((ROWS, RHS), BF16),
        in_specs=[inside, inside, inside],
        out_specs=anywhere,
        scratch_shapes=[vmem((ROWS, RHS), BF16), pltpu.SemaphoreType.DMA((ROWS // STEP,))],
        compiler_params=pltpu.CompilerParams(vmem_limit_bytes=16 * 1024 * 1024),
    )(*held)


def solution(mesh):
    torus = Mesh(mesh.devices.reshape(4, 16, 4, 2), AXES)
    placed = (P(AXES, None), P(AXES), P(AXES, None), P(None, None, AXES), P(None, None, AXES), P())
    return jax.shard_map(per_device, mesh=torus, in_specs=placed, out_specs=P(AXES, None), check_vma=False)
```
